32 devices in a mesh: seq: 8 (over z, x), head: 4 (over y, core).
Axes of the slice: x: 2, y: 2, z: 4, core: 2. Of those that a mesh axis runs over, the one named last changes fastest.
Arguments:
- query_in: bfloat16 [2048, 8192], P('seq', 'head'), may hold values from -1.796875 to 1.796875
- key_in: bfloat16 [2048, 8192], P('seq', 'head'), may hold values from -1.796875 to 1.796875
- value_in: bfloat16 [2048, 8192], P('seq', 'head'), may hold values from -11 to 11
- log_decay: float32 [2048, 64], P('seq', 'head'), may hold values from -1 to 0, as said below
- norm_gain: float32 [8192], P('head'), may hold values from 0.5 to 1.5
- prompt_lengths: int32 [4], replicated, may hold values from 1 to 1536, 2048 in all
- step_query: bfloat16 [4, 128, 8192], P(None, 'seq', 'head'), may hold values from -1.796875 to 1.796875
- step_key: bfloat16 [4, 128, 8192], P(None, 'seq', 'head'), may hold values from -1.796875 to 1.796875
- step_value: bfloat16 [4, 128, 8192], P(None, 'seq', 'head'), may hold values from -6 to 6
- step_decay: float32 [4, 128, 64], P(None, 'seq', 'head'), may hold values from -0.3 to -0.01
- row_prompt: int32 [128], P('seq'), may hold values from 0 to 3
Outputs:
- attn_out: bfloat16 [2048, 8192], P('seq', 'head')
- decode_out: bfloat16 [4, 128, 8192], P(None, 'seq', 'head')
The draws below stay inside these ranges and needn't reach their ends.
Inputs may be any that keep to these rules, and one draw needn't show every extreme that they name: `log_decay`: Negative; per head and token.
All inputs are finite; a program needn't handle non-finite values.
Results may differ from the reference program's by a relative error of at most 0.0056.
Values sent between devices are 32-bit elements; how exact they have to be, the bound alone decides.
A program may use at most 64 MiB of HBM per device.

```python
import math
import jax
import jax.numpy as jnp
import numpy as np
from jax import lax

HEAD_COUNT = 64
HDIM = 128
TOK_DEV = 256
BLOCK = 256
PROMPTS = 4
STEPS = 4
PROMPT_TOKENS = 2048
ROWS = 128


def draw_log_decay(key, part):
    fragments = jax.random.split(jax.random.fold_in(key, 11), 7)
    order = jax.random.permutation(fragments[0], HEAD_COUNT)
    fast = order < HEAD_COUNT // 2
    slow_rate = jnp.exp(jax.random.uniform(fragments[1], (HEAD_COUNT,), jnp.float32, jnp.log(0.2), jnp.log(1.0))) / PROMPT_TOKENS
    fast_rate = jnp.exp(jax.random.uniform(fragments[2], (HEAD_COUNT,), jnp.float32, jnp.log(1.0 / 50.0), jnp.log(1.0 / 30.0)))
    decay_rate = jnp.where(fast, fast_rate, slow_rate)
    spans = PROMPT_TOKENS // TOK_DEV
    device_multiplier = jnp.exp(jax.random.uniform(fragments[3], (spans, HEAD_COUNT), jnp.float32, -0.7, 0.7))
    device_multiplier = jnp.repeat(device_multiplier, TOK_DEV, axis=0)
    coarse_estimate = jax.random.uniform(fragments[4], (PROMPT_TOKENS, HEAD_COUNT), jnp.float32, 0.5, 1.5)
    spike_positions = jax.random.randint(fragments[5], (4,), 0, PROMPT_TOKENS)
    marked_rows = jnp.any(jnp.arange(PROMPT_TOKENS)[:, None] == spike_positions[None, :], axis=1)
    spike_group = jnp.log(jax.random.uniform(fragments[6], (PROMPT_TOKENS, HEAD_COUNT), jnp.float32, 0.5, 0.8))
    return (-decay_rate[None, :] * device_multiplier * coarse_estimate + jnp.where(marked_rows[:, None], spike_group, 0.0)).astype(jnp.float32)


def draw_value_in(key, part):
    fragments = jax.random.split(jax.random.fold_in(key, 23), 1)
    head_of = (jnp.arange(HEAD_COUNT * HDIM) // HDIM).astype(jnp.float32)
    scale = 0.5 * 3.0 ** (head_of / max(HEAD_COUNT - 1, 1))
    base = jnp.clip(jax.random.normal(fragments[0], (PROMPT_TOKENS, HEAD_COUNT * HDIM), jnp.float32), -4.0, 4.0)
    return (base * scale[None, :]).astype(jnp.bfloat16)


def place_ends(result, own_key, least, top_value):
    longest = result.shape.index(max(result.shape))
    spots = []
    for shift in (0, 1):
        where = [jax.random.randint(jax.random.fold_in(own_key, axis), (), 0, length) for axis, length in enumerate(result.shape)]
        where[longest] = (where[longest] + shift) % result.shape[longest]
        spots.append(tuple(where))
    return result.at[spots[0]].set(least).at[spots[1]].set(top_value)


def shard_levels(stream_key, dims, pieces, low, top_value):
    level = 1.0
    for position, parts in pieces:
        heights = jax.random.uniform(jax.random.fold_in(jax.random.fold_in(stream_key, 6), position), (parts,), jnp.float32, low / len(pieces), top_value / len(pieces))
        level = level * jnp.repeat(jnp.exp(heights), dims[position] // parts).reshape((-1,) + (1,) * (len(dims) - 1 - position))
    return level


def split_up(count, total, limit, lean):
    portions = [(1 << 20) // math.isqrt(grade ** lean) + 1 for grade in range(2, count + 1)]
    spare, counts = total - limit - (count - 1), [1] * (count - 1)
    while spare > 0:
        candidates = [i for i in range(count - 1) if counts[i] < limit]
        mass, remaining = sum([portions[i] for i in candidates]), spare
        for i in candidates:
            more = min(limit - counts[i], max(1, remaining * portions[i] // mass), spare)
            counts[i] = counts[i] + more
            spare = spare - more
    return np.array([limit] + counts)


def ragged_sizes(own_key, count, total, bound, lean):
    if count == 2:
        one = jax.random.randint(own_key, (), max(1, total - bound), min(bound, total - 1) + 1)
        return jnp.stack([one, total - one])
    sizes = jnp.asarray(split_up(count, total, bound, lean), jnp.int32)
    pairs = (count - 1) // 2
    giver, sink = sizes[1:1 + 2 * pairs:2], sizes[2:2 + 2 * pairs:2]
    margin = jnp.minimum(giver - 1, bound - sink)
    moved = jax.random.randint(jax.random.fold_in(own_key, 1), (pairs,), 0, 1 << 20) % (margin + 1)
    sizes = sizes.at[1:1 + 2 * pairs:2].set(giver - moved).at[2:2 + 2 * pairs:2].set(sink + moved)
    return sizes[jax.random.permutation(jax.random.fold_in(own_key, 2), count)]


def gaussian(rng, dims, scale, most, pieces=(), kind=jnp.bfloat16):
    values = scale * jax.random.normal(rng, dims, jnp.float32)
    if pieces:
        values = values * shard_levels(rng, dims, pieces, -0.22, 0.18)
    return jnp.clip(values, -most, most).astype(kind)


def setup_inputs(seed: int = 0) -> dict:
    streams_of = jax.random.split(jax.random.key(seed), 12)
    return {
        "query_in": gaussian(streams_of[0], (PROMPT_TOKENS, HEAD_COUNT * HDIM), 0.3, 1.796875, ((0, 8), (1, 4))),
        "key_in": gaussian(streams_of[1], (PROMPT_TOKENS, HEAD_COUNT * HDIM), 0.3, 1.796875, ((0, 8), (1, 4))),
        "value_in": draw_value_in(jax.random.fold_in(streams_of[11], 71), 0),
        "log_decay": draw_log_decay(jax.random.fold_in(streams_of[11], 71), 0),
        "norm_gain": jnp.clip(1.0 + 0.1 * jax.random.normal(streams_of[4], (HEAD_COUNT * HDIM,), jnp.float32), 0.5, 1.5),
        "prompt_lengths": ragged_sizes(streams_of[5], PROMPTS, PROMPT_TOKENS, PROMPT_TOKENS * 3 // 4, 2).astype(jnp.int32),
        "step_query": gaussian(streams_of[6], (STEPS, ROWS, HEAD_COUNT * HDIM), 0.3, 1.796875, ((1, 8), (2, 4))),
        "step_key": gaussian(streams_of[7], (STEPS, ROWS, HEAD_COUNT * HDIM), 0.3, 1.796875, ((1, 8), (2, 4))),
        "step_value": gaussian(streams_of[8], (STEPS, ROWS, HEAD_COUNT * HDIM), 1.0, 6.0, ((1, 8), (2, 4))),
        "step_decay": jnp.clip(-0.3 + 0.29000001 * jax.random.uniform(streams_of[9], (STEPS, ROWS, HEAD_COUNT), jnp.float32) ** shard_levels(streams_of[9], (STEPS, ROWS, HEAD_COUNT), ((1, 8), (2, 4)), -0.2, 0.2), -0.3, -0.01),
        "row_prompt": place_ends(jax.random.randint(streams_of[10], (ROWS,), 0, PROMPTS), jax.random.fold_in(streams_of[10], 1), 0, PROMPTS - 1).astype(jnp.int32),
    }


EPSILON = 1e-06

def segment_ids(prompt_lengths, positions):
    boundary = jnp.cumsum(prompt_lengths).astype(jnp.int32)
    return lax.optimization_barrier(jnp.sum((positions[:, None] >= boundary[None, :]).astype(jnp.int32), axis=1)).astype(jnp.int32)

def half_round(array):
    return lax.optimization_barrier(array.astype(jnp.bfloat16)).astype(jnp.float32)

def block_pass(query_blk, key_blk, value_blk, decay_blk, seg_blk, seg_front, state):
    cumul = jnp.cumsum(decay_blk, axis=0)
    length = seg_blk.shape[0]
    causal = jnp.arange(length)[:, None] >= jnp.arange(length)[None, :]
    linked = causal & (seg_blk[:, None] == seg_blk[None, :])
    spread = cumul[:, None, :] - cumul[None, :, :]
    factor = jnp.where(linked[:, :, None], jnp.exp(jnp.where(linked[:, :, None], spread, 0.0)), 0.0)
    query_f = query_blk.astype(jnp.float32)
    key_f = key_blk.astype(jnp.float32)
    value_f = value_blk.astype(jnp.float32)
    scores = jnp.einsum('thd,shd->hts', query_f, key_f)
    weights = half_round(scores * jnp.transpose(factor, (2, 0, 1)))
    inner = jnp.einsum('hts,shd->thd', weights, value_f)
    carried = jnp.exp(cumul) * (seg_blk == seg_front).astype(jnp.float32)[:, None]
    state_half = half_round(state)
    outer = jnp.einsum('thd,hde->the', query_f, state_half) * carried[:, :, None]
    keep = jnp.exp(cumul[-1:] - cumul) * (seg_blk == seg_blk[-1]).astype(jnp.float32)[:, None]
    keyed = half_round(key_f * keep[:, :, None])
    update = jnp.einsum('shd,she->hde', keyed, value_f)
    onward = jnp.exp(cumul[-1]) * (seg_blk[-1] == seg_front).astype(jnp.float32)
    new_state = onward[:, None, None] * state + update
    return (inner + outer, new_state)

def reference(query_in, key_in, value_in, log_decay, norm_gain, prompt_lengths, step_query, step_key, step_value, step_decay, row_prompt):
    nblocks = PROMPT_TOKENS // BLOCK
    positions = jnp.arange(PROMPT_TOKENS, dtype=jnp.int32)
    segs = segment_ids(prompt_lengths, positions)
    seg_prior = jnp.concatenate([jnp.full((1,), -1, jnp.int32), segs[:-1]]).astype(jnp.int32)
    shape4 = (nblocks, BLOCK, HEAD_COUNT, HDIM)
    inputs = (query_in.reshape(shape4), key_in.reshape(shape4), value_in.reshape(shape4), log_decay.reshape(nblocks, BLOCK, HEAD_COUNT), segs.reshape(nblocks, BLOCK), seg_prior.reshape(nblocks, BLOCK)[:, 0])

    def stepper(state, fragments):
        mixed_blk, new_state = block_pass(fragments[0], fragments[1], fragments[2], fragments[3], fragments[4], fragments[5], state)
        return (new_state, (mixed_blk, state))
    initial = jnp.zeros((HEAD_COUNT, HDIM, HDIM), jnp.float32)
    final_state, (mixed_all, starts) = lax.scan(stepper, initial, inputs)
    mixed = mixed_all.reshape(PROMPT_TOKENS, HEAD_COUNT * HDIM)
    scale = lax.rsqrt(lax.optimization_barrier(jnp.sum(mixed * mixed, axis=1)) / (HEAD_COUNT * HDIM) + EPSILON)
    attn_out = (mixed * scale[:, None] * norm_gain[None, :]).astype(jnp.bfloat16)
    boundary = jnp.cumsum(prompt_lengths).astype(jnp.int32)

    def prompt_end(prompt):
        last_tok = (boundary[prompt] - 1).astype(jnp.int32)
        blk_index = (last_tok // BLOCK).astype(jnp.int32)
        offset = (last_tok - blk_index * BLOCK).astype(jnp.int32)
        begin = (blk_index * BLOCK).astype(jnp.int32)
        key_blk = lax.dynamic_slice_in_dim(key_in, begin, BLOCK, 0).reshape(BLOCK, HEAD_COUNT, HDIM).astype(jnp.float32)
        value_blk = lax.dynamic_slice_in_dim(value_in, begin, BLOCK, 0).reshape(BLOCK, HEAD_COUNT, HDIM).astype(jnp.float32)
        decay_blk = lax.dynamic_slice_in_dim(log_decay, begin, BLOCK, 0)
        seg_blk = lax.dynamic_slice_in_dim(segs, begin, BLOCK, 0)
        seg_front = seg_prior[begin]
        cumul = jnp.cumsum(decay_blk, axis=0)
        reached = cumul[offset]
        taken = (jnp.arange(BLOCK) <= offset) & (seg_blk == prompt)
        keep_end = jnp.exp(jnp.where(taken[:, None], reached[None, :] - cumul, 0.0)) * taken.astype(jnp.float32)[:, None]
        tailed = half_round(key_blk * keep_end[:, :, None])
        part = jnp.einsum('shd,she->hde', tailed, value_blk)
        lead = jnp.exp(reached) * (seg_front == prompt).astype(jnp.float32)
        return lead[:, None, None] * starts[blk_index] + part
    prompt_state = lax.map(prompt_end, jnp.arange(PROMPTS, dtype=jnp.int32))

    def decode_row(fragments):
        prompt, queries, keyset, valueset, decays = fragments
        row_state = prompt_state[prompt]
        results = []
        for section in range(STEPS):
            query_now = queries[section].astype(jnp.float32).reshape(HEAD_COUNT, HDIM)
            key_now = keyset[section].astype(jnp.float32).reshape(HEAD_COUNT, HDIM)
            value_now = valueset[section].astype(jnp.float32).reshape(HEAD_COUNT, HDIM)
            row_state = jnp.exp(decays[section])[:, None, None] * row_state + key_now[:, :, None] * value_now[:, None, :]
            results.append(jnp.einsum('hd,hde->he', query_now, row_state, precision=lax.Precision.HIGHEST).reshape(HEAD_COUNT * HDIM))
        return jnp.stack(results)
    decoded = lax.map(decode_row, (row_prompt, jnp.transpose(step_query, (1, 0, 2)), jnp.transpose(step_key, (1, 0, 2)), jnp.transpose(step_value, (1, 0, 2)), jnp.transpose(step_decay, (1, 0, 2))))
    decoded = jnp.transpose(decoded, (1, 0, 2))
    step_scale = lax.rsqrt(lax.optimization_barrier(jnp.sum(decoded * decoded, axis=2)) / (HEAD_COUNT * HDIM) + EPSILON)
    decode_out = (decoded * step_scale[:, :, None] * norm_gain[None, None, :]).astype(jnp.bfloat16)
    return (attn_out, decode_out)
```

```python
import functools

import jax
import jax.numpy as jnp
from jax import lax
from jax.experimental import pallas as pl
from jax.experimental.pallas import tpu as pltpu
from jax.sharding import PartitionSpec as P

HDIM = 128
PROMPTS = 4
PAIR = 2
LAG = 3
AHEAD = 3
CUM_ROW = 4
CARRIED_ROW = 5

EPSILON = 1e-06
MESH = pl.DeviceIdType.MESH


def fused_kernel(
    n,
    n_head,
    steps,
    parts,
    fwd,
    bwd,
    lens_ref,
    prompt_ref,
    query_ref,
    key_ref,
    value_ref,
    decay_ref,
    gain_ref,
    sq_ref,
    sk_ref,
    sv_ref,
    sd_ref,
    attn_ref,
    out_ref,
    token_s,
    bias_s,
    weight_s,
    coef_s,
    coef_recv,
    row_s,
    row_recv,
    mixed_s,
    dec_s,
    own_part,
    x_send,
    x_recv,
    q_send,
    q_recv,
    f_recv,
    f_send,
    b_recv,
    b_send,
    pair_part,
    low_part,
    t_recv,
    t_send,
    e_mine,
    acc_sq,
    acc_dsq,
    acc_own,
    e_send,
    e_recv,
    r_send,
    r_recv,
    n_send,
    n_recv,
    d_send,
    d_recv,
    xs_sem,
    xr_sem,
    cs_sem,
    cr_sem,
    qs_sem,
    qr_sem,
    ws_sem,
    wr_sem,
    fs_sem,
    fr_sem,
    bs_sem,
    br_sem,
    ts_sem,
    tr_sem,
    es_sem,
    er_sem,
    rs_sem,
    rr_sem,
    ns_sem,
    nr_sem,
    ds_sem,
    dr_sem,
):
    f32, bf16, i32 = jnp.float32, jnp.bfloat16, jnp.int32
    me = lax.axis_index("seq")
    hd = lax.axis_index("head")
    side = lax.rem(me, PAIR)
    rank = lax.div(me, PAIR)
    ranks = n // PAIR
    partner = me + 1 - 2 * side
    half = own_part.shape[0]
    heads = PAIR * half
    tok, width = query_ref.shape
    slots = PROMPTS
    units = half * slots
    rows = sq_ref.shape[0] // steps
    mine = side * half
    theirs = (1 - side) * half
    is_first = rank == 0
    is_last = rank == ranks - 1
    low = side == 0
    ahead = lax.rem(me + PAIR, n)
    behind = lax.rem(me + n - PAIR, n)

    def copy(src, dst, send, recv, to):
        return pltpu.make_async_remote_copy(
            src_ref=src,
            dst_ref=dst,
            send_sem=send,
            recv_sem=recv,
            device_id=to,
            device_id_type=MESH,
        )

    def x_copy(j, k):
        i = j * parts + k
        return copy(
            x_send.at[j, k], x_recv.at[j, k], xs_sem.at[i], xr_sem.at[i], {"seq": partner}
        )

    def f_copy(j, p):
        i = j * slots + p
        return copy(f_send.at[j, p], f_recv.at[j, p], fs_sem.at[i], fr_sem.at[i], {"seq": ahead})

    def b_copy(j, p):
        i = j * slots + p
        return copy(b_send.at[j, p], b_recv.at[j, p], bs_sem.at[i], br_sem.at[i], {"seq": behind})

    def q_copy(j):
        return copy(q_send.at[j], q_recv.at[j], qs_sem.at[j], qr_sem.at[j], {"seq": partner})

    def e_copy(j):
        return copy(e_send.at[j], e_recv.at[j], es_sem.at[j], er_sem.at[j], {"seq": partner})

    def r_copy(j):
        return copy(r_send.at[j], r_recv.at[j], rs_sem.at[j], rr_sem.at[j], {"seq": partner})

    def peer(k):
        return {"head": lax.rem(hd + k, n_head)}

    def n_copy(k):
        return copy(n_send, n_recv.at[k - 1], ns_sem.at[k - 1], nr_sem.at[k - 1], peer(k))

    def d_copy(k):
        return copy(d_send, d_recv.at[k - 1], ds_sem.at[k - 1], dr_sem.at[k - 1], peer(k))

    coef_copy = copy(coef_s.at[1 - side], coef_recv, cs_sem, cr_sem, {"seq": partner})
    row_copy = copy(row_s, row_recv, ws_sem, wr_sem, {"seq": partner})
    t_copy = copy(t_send, t_recv, ts_sem, tr_sem, {"seq": behind})

    def lanes(h):
        return pl.ds(pl.multiple_of(h * HDIM, HDIM), HDIM)

    barrier = pltpu.get_barrier_semaphore()

    def greet(to):
        pl.semaphore_signal(barrier, inc=1, device_id=to, device_id_type=MESH)

    greet({"seq": partner})
    for k in range(1, n_head):
        greet(peer(k))

    @pl.when(jnp.logical_not(is_last))
    def _():
        greet({"seq": ahead})

    @pl.when(jnp.logical_not(is_first))
    def _():
        greet({"seq": behind})

    ends = []
    for p in range(slots):
        ends.append(lens_ref[p] + (ends[-1] if p else 0))
    begins = [ends[p] - lens_ref[p] for p in range(slots)]

    def number(flag):
        return jnp.where(flag, 1, 0).astype(i32)

    def unity(flag):
        return jnp.where(flag, 1.0, 0.0).astype(f32)

    def seg_of(token):
        total = number(token >= ends[0])
        for p in range(1, slots):
            total = total + number(token >= ends[p])
        return total

    def seg_before(token):
        return jnp.where(token > 0, seg_of(token - 1), -1)

    first = me * tok
    pair_first = rank * (PAIR * tok)
    base = seg_of(first)
    base_low = seg_of(pair_first)
    base_high = seg_of(pair_first + tok)
    front_low = seg_before(pair_first)
    front_high = seg_before(pair_first + tok)

    sub = lax.broadcasted_iota(i32, (tok, tok), 0)
    lane = lax.broadcasted_iota(i32, (tok, tok), 1)
    cum = jnp.dot(
        decay_ref[...],
        jnp.where(sub <= lane, 1.0, 0.0).astype(f32),
        precision=lax.Precision.HIGHEST,
        preferred_element_type=f32,
    )
    place = lax.broadcasted_iota(i32, (heads, tok), 1)
    segs = seg_of(place + first)
    goal = jnp.zeros_like(cum)
    for p in range(slots):
        last = jnp.clip(ends[p] - first, 1, tok) - 1
        reached = jnp.sum(jnp.where(place == last, cum, 0.0), axis=1, keepdims=True)
        goal = jnp.where(segs == p, reached, goal)
        grown = jnp.where(begins[p] < first, jnp.exp(reached), 0.0)
        coef = jnp.where(ends[p] <= first, 1.0, grown)
        coef = jnp.broadcast_to(coef, (heads, HDIM))
        for s in range(PAIR):
            coef_s[s, p] = coef[s * half : (s + 1) * half]
    keep = jnp.exp(goal - cum)
    carried = jnp.where(segs == seg_before(first), jnp.exp(cum), 0.0)
    keeps = [jnp.where(segs == base + k, keep, 0.0) for k in range(parts)]
    token_s[...] = jnp.zeros_like(token_s)
    for h in range(heads):
        at = slice(h, h + 1)
        for k in range(parts):
            token_s[h, k : k + 1, :] = keeps[k][at]
        token_s[h, CUM_ROW : CUM_ROW + 1, :] = cum[at]
        token_s[h, CARRIED_ROW : CARRIED_ROW + 1, :] = carried[at]

    def make_parts(h, j, into):
        key = key_ref[:, lanes(h)].astype(f32)
        value = value_ref[:, lanes(h)]
        cols = jnp.transpose(token_s[h])
        for k in range(parts):
            keyed = (key * cols[:, k : k + 1]).astype(bf16)
            into[j, k] = lax.dot_general(
                keyed, value, (((0,), (0,)), ((), ())), preferred_element_type=f32
            )

    def within(h):
        query = query_ref[:, lanes(h)]
        scores = lax.dot_general(
            query, key_ref[:, lanes(h)], (((1,), (1,)), ((), ())), preferred_element_type=f32
        )
        cols = jnp.transpose(token_s[h])
        column = cols[:, CUM_ROW : CUM_ROW + 1]
        spread = column - token_s[h, CUM_ROW : CUM_ROW + 1, :] + bias_s[...]
        weights = (scores * jnp.exp(spread)).astype(bf16)
        mixed_s[:, lanes(h)] = jnp.dot(
            weights, value_ref[:, lanes(h)], preferred_element_type=f32
        )

    def across(h, entry):
        column = jnp.transpose(token_s[h])[:, CARRIED_ROW : CARRIED_ROW + 1]
        outer = jnp.dot(query_ref[:, lanes(h)], entry.astype(bf16), preferred_element_type=f32)
        mixed = mixed_s[:, lanes(h)] + outer * column
        mixed_s[:, lanes(h)] = mixed
        acc_sq[...] += mixed * mixed

    pick = lax.broadcasted_iota(i32, (rows, heads), 1)

    def weight_col(i, h):
        return jnp.sum(jnp.where(pick == h, weight_s[i], 0.0), axis=1, keepdims=True)

    def own_steps(h):
        query = sq_ref[:, lanes(h)].astype(f32)
        key = sk_ref[:, lanes(h)].astype(f32)
        value = sv_ref[:, lanes(h)].astype(f32)
        cut = lambda a, i: a[i * rows : (i + 1) * rows]
        spot = steps
        for i in range(steps):
            total = None
            for j in range(i + 1):
                dot = jnp.sum(cut(query, i) * cut(key, j), axis=1, keepdims=True)
                if j < i:
                    dot = dot * weight_col(spot, h)
                    spot += 1
                term = dot * cut(value, j)
                total = term if j == 0 else total + term
            dec_s[i * rows : (i + 1) * rows, lanes(h)] = total

    def from_state(h, product):
        for i in range(steps):
            at = slice(i * rows, (i + 1) * rows)
            out = dec_s[at, lanes(h)] + weight_col(i, h) * product[at]
            dec_s[at, lanes(h)] = out
            acc_dsq[at] += out * out

    def send_parts(j):
        make_parts(theirs + j, j, x_send)
        for k in range(parts):
            x_copy(j, k).start()

    make_parts(theirs, 0, x_send)
    pl.semaphore_wait(
        barrier, n_head + jnp.where(is_first, 0, 1) + jnp.where(is_last, 0, 1)
    )
    coef_copy.start()
    for k in range(parts):
        x_copy(0, k).start()
    for j in range(1, AHEAD):
        send_parts(j)
    make_parts(mine, 0, own_part)

    column = lax.broadcasted_iota(i32, (rows, HDIM), 0)
    marks = jnp.zeros((rows, HDIM), f32)
    for r in range(rows):
        marks = jnp.where(column == r, prompt_ref[r].astype(f32), marks)
    row_s[...] = marks
    row_copy.start()
    tops = jnp.broadcast_to(segs[0:1].astype(f32), (8, tok))
    linked = (sub >= lane) & (jnp.transpose(tops)[:, 0:1] == tops[0:1])
    bias_s[...] = jnp.where(linked, 0.0, -jnp.inf)
    totals = []
    for i in range(steps):
        totals.append(sd_ref[i] + totals[-1] if i else sd_ref[i])
    spot = steps
    for i in range(steps):
        weight_s[i] = jnp.exp(totals[i])
        for j in range(i):
            weight_s[spot] = jnp.exp(totals[i] - totals[j])
            spot += 1
    acc_sq[...] = jnp.zeros_like(acc_sq)
    acc_dsq[...] = jnp.zeros_like(acc_dsq)
    if fwd < slots:
        f_recv[:, fwd:] = jnp.zeros((half, slots - fwd, HDIM, HDIM), f32)
    if bwd > 0:
        b_recv[:, :bwd] = jnp.zeros((half, bwd, HDIM, HDIM), f32)

    @pl.when(is_first)
    def _():
        f_recv[:, :fwd] = jnp.zeros((half, fwd, HDIM, HDIM), f32)

    @pl.when(is_last)
    def _():
        b_recv[:, bwd:] = jnp.zeros((half, slots - bwd, HDIM, HDIM), f32)
        t_recv[...] = jnp.ones_like(t_recv)

    coef_copy.wait()
    row_copy.wait()

    lag_f = rank * LAG
    lag_b = (ranks - 1 - rank) * LAG
    lag_d = jnp.maximum(lag_f, lag_b)

    def relay_decay():
        @pl.when(jnp.logical_not(is_last))
        def _():
            t_copy.wait_recv()

        @pl.when(jnp.logical_not(is_first))
        def _():
            t_send[...] = t_recv[...] * coef_recv[...] * coef_s[side]
            t_copy.start()

    def rows_of(j, p):
        c_own = coef_s[side, p, pl.ds(j, 1), :]
        c_other = coef_recv[p, pl.ds(j, 1), :]
        return jnp.where(low, c_own, c_other), jnp.where(low, c_other, c_own)

    def combine(j, p):
        @pl.when(p == 0)
        def _():
            for k in range(parts):
                x_copy(j, k).wait_recv()

        base_own = jnp.where(low, base_low, base_high)
        base_other = jnp.where(low, base_high, base_low)
        own = None
        other = None
        for k in range(parts):
            a = unity(base_own + k == p) * own_part[j, k]
            b = unity(base_other + k == p) * x_recv[j, k]
            own = a if k == 0 else own + a
            other = b if k == 0 else other + b
        c_low, c_high = rows_of(j, p)
        at_low = jnp.where(low, own, other)
        low_part[j, p] = at_low
        pair_part[j, p] = c_high * at_low + jnp.where(low, other, own)

    def forward(j, p):
        @pl.when(jnp.logical_not(is_first) & (p < fwd))
        def _():
            f_copy(j, p).wait_recv()

        c_low, c_high = rows_of(j, p)
        came = f_recv[j, p]
        middle = c_low * came
        f_send[j, p] = c_high * middle + pair_part[j, p]

        @pl.when(jnp.logical_not(is_last) & (p < fwd))
        def _():
            f_copy(j, p).start()

        at_low = came * unity(front_low == p)
        at_high = (middle + low_part[j, p]) * unity(front_high == p)
        to_mine = jnp.where(low, at_low, at_high)
        to_theirs = jnp.where(low, at_high, at_low)

        @pl.when(p == 0)
        def _():
            e_mine[j] = to_mine
            e_send[j] = to_theirs

        @pl.when(p > 0)
        def _():
            e_mine[j] += to_mine
            e_send[j] += to_theirs

        @pl.when(p == slots - 1)
        def _():
            e_copy(j).start()

    def backward(j, p):
        @pl.when(jnp.logical_not(is_last) & (p >= bwd))
        def _():
            b_copy(j, p).wait_recv()

        @pl.when(jnp.logical_not(is_first) & (p >= bwd))
        def _():
            t_row = t_recv[p, pl.ds(j, 1), :]
            b_send[j, p] = b_recv[j, p] + t_row * pair_part[j, p]
            b_copy(j, p).start()

    def decode(j, p):
        @pl.when(p == 0)
        def _():
            q_copy(j).wait_recv()

        t_row = t_recv[p, pl.ds(j, 1), :]
        final = (t_row * f_send[j, p] + b_recv[j, p]).astype(bf16)
        got_own = jnp.dot(sq_ref[:, lanes(mine + j)], final, preferred_element_type=f32)
        got_other = jnp.dot(q_recv[j].astype(bf16), final, preferred_element_type=f32)
        slot = p.astype(f32)
        spread = lambda a: jnp.concatenate([a] * steps, axis=0)
        got_own = jnp.where(spread(row_s[...]) == slot, got_own, 0.0)
        got_other = jnp.where(spread(row_recv[...]) == slot, got_other, 0.0)

        @pl.when(p == 0)
        def _():
            acc_own[...] = got_own
            r_send[j] = got_other

        @pl.when(p > 0)
        def _():
            acc_own[...] += got_own
            r_send[j] += got_other

        @pl.when(p == slots - 1)
        def _():
            r_copy(j).start()
            from_state(mine + j, acc_own[...])

    def split(t):
        return lax.div(t, slots), lax.rem(t, slots)

    @pl.loop(0, units + (ranks - 1) * LAG)
    def _(t):
        j, p = split(t)

        @pl.when(t < units)
        def _():
            combine(j, p)

        @pl.when(t == lag_b)
        def _():
            relay_decay()

        @pl.when((t >= lag_f) & (t < units + lag_f))
        def _():
            forward(*split(t - lag_f))

        @pl.when((t >= lag_b) & (t < units + lag_b))
        def _():
            backward(*split(t - lag_b))

        @pl.when((t < units) & (p == 0))
        def _():
            q_send[j] = sq_ref[:, lanes(theirs + j)].astype(f32)
            q_copy(j).start()

            @pl.when(j < half - AHEAD)
            def _():
                send_parts(j + AHEAD)

        @pl.when((t < units) & (p == 1))
        def _():
            own_steps(mine + j)
            within(mine + j)

        @pl.when((t < units) & (p == 2))
        def _():
            own_steps(theirs + j)
            within(theirs + j)

            @pl.when(j < half - 1)
            def _():
                make_parts(mine + j + 1, j + 1, own_part)

        @pl.when((t >= lag_d) & (t < units + lag_d))
        def _():
            decode(*split(t - lag_d))

        @pl.when((t >= lag_f) & (t < units + lag_f))
        def _():
            jf, pf = split(t - lag_f)

            @pl.when(pf == slots - 1)
            def _():
                across(mine + jf, e_mine[jf])

    @pl.loop(0, half)
    def _(j):
        e_copy(j).wait()
        across(theirs + j, e_recv[j])

    def row_sums(acc):
        return lax.dot_general(
            jnp.ones((8, HDIM), f32),
            acc[...],
            (((1,), (1,)), ((), ())),
            precision=lax.Precision.HIGHEST,
            preferred_element_type=f32,
        )

    def scale_of(total):
        scale = lax.rsqrt(total / (n_head * width) + EPSILON)
        return jnp.transpose(scale)[:, 0:1]

    n_send[...] = row_sums(acc_sq)
    for k in range(1, n_head):
        n_copy(k).start()

    @pl.loop(0, half)
    def _(j):
        r_copy(j).wait()
        from_state(theirs + j, r_recv[j])

    d_send[...] = row_sums(acc_dsq)
    for k in range(1, n_head):
        d_copy(k).start()

    total = n_send[...]
    for k in range(1, n_head):
        n_copy(k).wait()
        total = total + n_recv[k - 1]
    scale = jnp.broadcast_to(scale_of(total), (tok, HDIM))

    @pl.loop(0, heads)
    def _(h):
        at = lanes(h)
        attn_ref[:, at] = (mixed_s[:, at] * scale * gain_ref[:, at]).astype(bf16)

    total = d_send[...]
    for k in range(1, n_head):
        d_copy(k).wait()
        total = total + d_recv[k - 1]
    dec_scale = scale_of(total)
    out_ref[...] = (dec_s[...] * dec_scale * gain_ref[...]).astype(bf16)

    @pl.loop(0, half)
    def _(j):
        q_copy(j).wait_send()
        for k in range(parts):
            x_copy(j, k).wait_send()

        for p in range(fwd):

            @pl.when(jnp.logical_not(is_last))
            def _():
                f_copy(j, p).wait_send()

        for p in range(bwd, slots):

            @pl.when(jnp.logical_not(is_first))
            def _():
                b_copy(j, p).wait_send()

    @pl.when(jnp.logical_not(is_first))
    def _():
        t_copy.wait_send()


def fused(n, n_head, steps, variant, collective, *operands):
    parts, fwd, bwd = variant
    query, decay, step, step_decay = operands[2], operands[5], operands[7], operands[10]
    tok, width = query.shape
    heads = decay.shape[0]
    half = heads // PAIR
    vectors = step.shape[0]
    rows = vectors // steps
    slots = PROMPTS
    f32, bf16 = jnp.float32, jnp.bfloat16
    vmem = pl.BlockSpec(memory_space=pltpu.VMEM)
    smem = pl.BlockSpec(memory_space=pltpu.SMEM)
    dma = pltpu.SemaphoreType.DMA
    buffer = lambda *shape: pltpu.VMEM(shape, f32)
    states = buffer(half, slots, HDIM, HDIM)
    pieces = buffer(half, parts, HDIM, HDIM)
    decays = buffer(slots, half, HDIM)
    entries = buffer(half, HDIM, HDIM)
    products = buffer(half, vectors, HDIM)
    return pl.pallas_call(
        functools.partial(fused_kernel, n, n_head, steps, parts, fwd, bwd),
        out_shape=(
            jax.ShapeDtypeStruct((tok, width), bf16),
            jax.ShapeDtypeStruct((vectors, width), bf16),
        ),
        in_specs=[smem] * 2 + [vmem] * (len(operands) - 2),
        out_specs=(vmem,) * 2,
        scratch_shapes=[
            buffer(heads, 8, tok),
            buffer(tok, tok),
            buffer(steps * (steps + 1) // 2, rows, heads),
            buffer(PAIR, slots, half, HDIM),
            decays,
            buffer(rows, HDIM),
            buffer(rows, HDIM),
            buffer(tok, width),
            buffer(vectors, width),
            pieces,
            pieces,
            pieces,
            products,
            products,
            states,
            states,
            states,
            states,
            states,
            states,
            decays,
            decays,
            entries,
            buffer(tok, HDIM),
            buffer(vectors, HDIM),
            buffer(vectors, HDIM),
            entries,
            entries,
            products,
            products,
            buffer(8, tok),
            buffer(n_head - 1, 8, tok),
            buffer(8, vectors),
            buffer(n_head - 1, 8, vectors),
            dma((half * parts,)),
            dma((half * parts,)),
            dma,
            dma,
            dma((half,)),
            dma((half,)),
            dma,
            dma,
            dma((half * slots,)),
            dma((half * slots,)),
            dma((half * slots,)),
            dma((half * slots,)),
            dma,
            dma,
            dma((half,)),
            dma((half,)),
            dma((half,)),
            dma((half,)),
            dma((n_head - 1,)),
            dma((n_head - 1,)),
            dma((n_head - 1,)),
            dma((n_head - 1,)),
        ],
        compiler_params=pltpu.CompilerParams(
            collective_id=collective, has_side_effects=True, vmem_limit_bytes=56 * 1024 * 1024
        ),
        name="fused",
    )(*operands)


def local(
    n,
    n_head,
    query_in,
    key_in,
    value_in,
    log_decay,
    norm_gain,
    prompt_lengths,
    step_query,
    step_key,
    step_value,
    step_decay,
    row_prompt,
):
    steps, rows = step_query.shape[:2]
    flat = lambda a: a.reshape(steps * rows, -1)
    attn_out, decode_out = fused(
        n,
        n_head,
        steps,
        (PROMPTS, PROMPTS, 0),
        0,
        prompt_lengths,
        row_prompt,
        query_in,
        key_in,
        value_in,
        log_decay.T,
        norm_gain[None, :],
        flat(step_query),
        flat(step_key),
        flat(step_value),
        step_decay,
    )
    return (attn_out, decode_out.reshape(step_query.shape))


def solution(mesh):
    in_specs = (
        P("seq", "head"),
        P("seq", "head"),
        P("seq", "head"),
        P("seq", "head"),
        P("head"),
        P(),
        P(None, "seq", "head"),
        P(None, "seq", "head"),
        P(None, "seq", "head"),
        P(None, "seq", "head"),
        P("seq"),
    )
    out_specs = (P("seq", "head"), P(None, "seq", "head"))
    return jax.shard_map(
        functools.partial(local, mesh.shape["seq"], mesh.shape["head"]),
        mesh=mesh,
        in_specs=in_specs,
        out_specs=out_specs,
        check_vma=False,
    )
```

```python
import functools

import jax
import jax.numpy as jnp
from jax import lax
from jax.experimental import pallas as pl
from jax.experimental.pallas import tpu as pltpu
from jax.sharding import PartitionSpec as P

HDIM = 128
PROMPTS = 4
PAIR = 2
LAG = 3
CUT = 1
AHEAD = 1
VARIANTS = ((2, 4, 0), (3, 4, 0), (2, 3, 1), (3, 3, 1), (4, 4, 0))
CUM_ROW = 4
CARRIED_ROW = 5

EPSILON = 1e-06
MESH = pl.DeviceIdType.MESH


def fused_kernel(
    n,
    n_head,
    steps,
    parts,
    fwd,
    bwd,
    lens_ref,
    prompt_ref,
    query_ref,
    key_ref,
    value_ref,
    decay_ref,
    gain_ref,
    sq_ref,
    sk_ref,
    sv_ref,
    sd_ref,
    attn_ref,
    out_ref,
    token_s,
    bias_s,
    weight_s,
    coef_s,
    coef_recv,
    row_s,
    row_recv,
    mixed_s,
    dec_s,
    own_part,
    x_send,
    x_recv,
    q_send,
    q_recv,
    f_recv,
    f_send,
    b_recv,
    b_send,
    pair_part,
    low_part,
    t_recv,
    t_send,
    e_mine,
    acc_sq,
    acc_dsq,
    acc_own,
    e_send,
    e_recv,
    r_send,
    r_recv,
    n_send,
    n_recv,
    d_send,
    d_recv,
    xs_sem,
    xr_sem,
    cs_sem,
    cr_sem,
    qs_sem,
    qr_sem,
    ws_sem,
    wr_sem,
    fs_sem,
    fr_sem,
    bs_sem,
    br_sem,
    ts_sem,
    tr_sem,
    es_sem,
    er_sem,
    rs_sem,
    rr_sem,
    ns_sem,
    nr_sem,
    ds_sem,
    dr_sem,
):
    f32, bf16, i32 = jnp.float32, jnp.bfloat16, jnp.int32
    me = lax.axis_index("seq")
    hd = lax.axis_index("head")
    side = lax.rem(me, PAIR)
    rank = lax.div(me, PAIR)
    ranks = n // PAIR
    partner = me + 1 - 2 * side
    half = own_part.shape[0]
    heads = PAIR * half
    tok, width = query_ref.shape
    slots = PROMPTS
    span = slots * CUT
    units = half * span
    cut = HDIM // CUT
    rows = sq_ref.shape[0] // steps
    mine = side * half
    theirs = (1 - side) * half
    is_first = rank == 0
    is_last = rank == ranks - 1
    low = side == 0
    ahead = lax.rem(me + PAIR, n)
    behind = lax.rem(me + n - PAIR, n)

    def copy(src, dst, send, recv, to):
        return pltpu.make_async_remote_copy(
            src_ref=src,
            dst_ref=dst,
            send_sem=send,
            recv_sem=recv,
            device_id=to,
            device_id_type=MESH,
        )

    def x_copy(j, k):
        i = j * parts + k
        return copy(
            x_send.at[j, k], x_recv.at[j, k], xs_sem.at[i], xr_sem.at[i], {"seq": partner}
        )

    def piece(c):
        return pl.ds(pl.multiple_of(c * cut, cut), cut)

    def f_copy(j, p, c):
        i, at = j * span + p * CUT + c, piece(c)
        return copy(
            f_send.at[j, p, at], f_recv.at[j, p, at], fs_sem.at[i], fr_sem.at[i], {"seq": ahead}
        )

    def b_copy(j, p, c):
        i, at = j * span + p * CUT + c, piece(c)
        return copy(
            b_send.at[j, p, at], b_recv.at[j, p, at], bs_sem.at[i], br_sem.at[i], {"seq": behind}
        )

    def q_copy(j):
        return copy(q_send.at[j], q_recv.at[j], qs_sem.at[j], qr_sem.at[j], {"seq": partner})

    def e_copy(j):
        return copy(e_send.at[j], e_recv.at[j], es_sem.at[j], er_sem.at[j], {"seq": partner})

    def r_copy(j):
        return copy(r_send.at[j], r_recv.at[j], rs_sem.at[j], rr_sem.at[j], {"seq": partner})

    def peer(k):
        return {"head": lax.rem(hd + k, n_head)}

    def n_copy(k):
        return copy(n_send, n_recv.at[k - 1], ns_sem.at[k - 1], nr_sem.at[k - 1], peer(k))

    def d_copy(k):
        return copy(d_send, d_recv.at[k - 1], ds_sem.at[k - 1], dr_sem.at[k - 1], peer(k))

    coef_copy = copy(coef_s.at[1 - side], coef_recv, cs_sem, cr_sem, {"seq": partner})
    row_copy = copy(row_s, row_recv, ws_sem, wr_sem, {"seq": partner})
    t_copy = copy(t_send, t_recv, ts_sem, tr_sem, {"seq": behind})

    def lanes(h):
        return pl.ds(pl.multiple_of(h * HDIM, HDIM), HDIM)

    barrier = pltpu.get_barrier_semaphore()

    def greet(to):
        pl.semaphore_signal(barrier, inc=1, device_id=to, device_id_type=MESH)

    greet({"seq": partner})
    for k in range(1, n_head):
        greet(peer(k))

    @pl.when(jnp.logical_not(is_last))
    def _():
        greet({"seq": ahead})

    @pl.when(jnp.logical_not(is_first))
    def _():
        greet({"seq": behind})

    ends = []
    for p in range(slots):
        ends.append(lens_ref[p] + (ends[-1] if p else 0))
    begins = [ends[p] - lens_ref[p] for p in range(slots)]

    def number(flag):
        return jnp.where(flag, 1, 0).astype(i32)

    def unity(flag):
        return jnp.where(flag, 1.0, 0.0).astype(f32)

    def seg_of(token):
        total = number(token >= ends[0])
        for p in range(1, slots):
            total = total + number(token >= ends[p])
        return total

    def seg_before(token):
        return jnp.where(token > 0, seg_of(token - 1), -1)

    first = me * tok
    pair_first = rank * (PAIR * tok)
    base = seg_of(first)
    base_low = seg_of(pair_first)
    base_high = seg_of(pair_first + tok)
    front_low = seg_before(pair_first)
    front_high = seg_before(pair_first + tok)

    sub = lax.broadcasted_iota(i32, (tok, tok), 0)
    lane = lax.broadcasted_iota(i32, (tok, tok), 1)
    cum = jnp.dot(
        decay_ref[...],
        jnp.where(sub <= lane, 1.0, 0.0).astype(f32),
        precision=lax.Precision.HIGHEST,
        preferred_element_type=f32,
    )
    place = lax.broadcasted_iota(i32, (heads, tok), 1)
    segs = seg_of(place + first)
    goal = jnp.zeros_like(cum)
    for p in range(slots):
        last = jnp.clip(ends[p] - first, 1, tok) - 1
        reached = jnp.sum(jnp.where(place == last, cum, 0.0), axis=1, keepdims=True)
        goal = jnp.where(segs == p, reached, goal)
        grown = jnp.where(begins[p] < first, jnp.exp(reached), 0.0)
        coef = jnp.where(ends[p] <= first, 1.0, grown)
        coef = jnp.broadcast_to(coef, (heads, HDIM))
        for s in range(PAIR):
            coef_s[s, p] = coef[s * half : (s + 1) * half]
    keep = jnp.exp(goal - cum)
    carried = jnp.where(segs == seg_before(first), jnp.exp(cum), 0.0)
    keeps = [jnp.where(segs == base + k, keep, 0.0) for k in range(parts)]
    token_s[...] = jnp.zeros_like(token_s)
    for h in range(heads):
        at = slice(h, h + 1)
        for k in range(parts):
            token_s[h, k : k + 1, :] = keeps[k][at]
        token_s[h, CUM_ROW : CUM_ROW + 1, :] = cum[at]
        token_s[h, CARRIED_ROW : CARRIED_ROW + 1, :] = carried[at]

    def make_parts(h, j, into):
        key = key_ref[:, lanes(h)].astype(f32)
        value = value_ref[:, lanes(h)]
        cols = jnp.transpose(token_s[h])
        for k in range(parts):
            keyed = (key * cols[:, k : k + 1]).astype(bf16)
            into[j, k] = lax.dot_general(
                keyed, value, (((0,), (0,)), ((), ())), preferred_element_type=f32
            )

    def within(h):
        query = query_ref[:, lanes(h)]
        scores = lax.dot_general(
            query, key_ref[:, lanes(h)], (((1,), (1,)), ((), ())), preferred_element_type=f32
        )
        cols = jnp.transpose(token_s[h])
        column = cols[:, CUM_ROW : CUM_ROW + 1]
        spread = column - token_s[h, CUM_ROW : CUM_ROW + 1, :] + bias_s[...]
        weights = (scores * jnp.exp(spread)).astype(bf16)
        mixed_s[:, lanes(h)] = jnp.dot(
            weights, value_ref[:, lanes(h)], preferred_element_type=f32
        )

    def across(h, entry):
        column = jnp.transpose(token_s[h])[:, CARRIED_ROW : CARRIED_ROW + 1]
        outer = jnp.dot(query_ref[:, lanes(h)], entry.astype(bf16), preferred_element_type=f32)
        mixed = mixed_s[:, lanes(h)] + outer * column
        mixed_s[:, lanes(h)] = mixed
        acc_sq[...] += mixed * mixed

    pick = lax.broadcasted_iota(i32, (rows, heads), 1)

    def weight_col(i, h):
        return jnp.sum(jnp.where(pick == h, weight_s[i], 0.0), axis=1, keepdims=True)

    def own_steps(h):
        query = sq_ref[:, lanes(h)].astype(f32)
        key = sk_ref[:, lanes(h)].astype(f32)
        value = sv_ref[:, lanes(h)].astype(f32)
        step = lambda a, i: a[i * rows : (i + 1) * rows]
        spot = steps
        for i in range(steps):
            total = None
            for j in range(i + 1):
                dot = jnp.sum(step(query, i) * step(key, j), axis=1, keepdims=True)
                if j < i:
                    dot = dot * weight_col(spot, h)
                    spot += 1
                term = dot * step(value, j)
                total = term if j == 0 else total + term
            dec_s[i * rows : (i + 1) * rows, lanes(h)] = total

    def from_state(h, product):
        for i in range(steps):
            at = slice(i * rows, (i + 1) * rows)
            out = dec_s[at, lanes(h)] + weight_col(i, h) * product[at]
            dec_s[at, lanes(h)] = out
            acc_dsq[at] += out * out

    def send_parts(j):
        make_parts(theirs + j, j, x_send)
        for k in range(parts):
            x_copy(j, k).start()
        send_query(j)

    def send_query(j):
        q_send[j] = sq_ref[:, lanes(theirs + j)].astype(f32)
        q_copy(j).start()

    make_parts(theirs, 0, x_send)
    pl.semaphore_wait(
        barrier, n_head + jnp.where(is_first, 0, 1) + jnp.where(is_last, 0, 1)
    )
    coef_copy.start()
    for k in range(parts):
        x_copy(0, k).start()
    send_query(0)
    pl.loop(1, AHEAD)(send_parts)
    make_parts(mine, 0, own_part)

    column = lax.broadcasted_iota(i32, (rows, HDIM), 0)
    marks = jnp.zeros((rows, HDIM), f32)
    for r in range(rows):
        marks = jnp.where(column == r, prompt_ref[r].astype(f32), marks)
    row_s[...] = marks
    row_copy.start()
    tops = jnp.broadcast_to(segs[0:1].astype(f32), (8, tok))
    linked = (sub >= lane) & (jnp.transpose(tops)[:, 0:1] == tops[0:1])
    bias_s[...] = jnp.where(linked, 0.0, -jnp.inf)
    totals = []
    for i in range(steps):
        totals.append(sd_ref[i] + totals[-1] if i else sd_ref[i])
    spot = steps
    for i in range(steps):
        weight_s[i] = jnp.exp(totals[i])
        for j in range(i):
            weight_s[spot] = jnp.exp(totals[i] - totals[j])
            spot += 1
    acc_sq[...] = jnp.zeros_like(acc_sq)
    acc_dsq[...] = jnp.zeros_like(acc_dsq)
    if fwd < slots:
        f_recv[:, fwd:] = jnp.zeros((half, slots - fwd, HDIM, HDIM), f32)
    if bwd > 0:
        b_recv[:, :bwd] = jnp.zeros((half, bwd, HDIM, HDIM), f32)

    @pl.when(is_first)
    def _():
        f_recv[:, :fwd] = jnp.zeros((half, fwd, HDIM, HDIM), f32)

    @pl.when(is_last)
    def _():
        b_recv[:, bwd:] = jnp.zeros((half, slots - bwd, HDIM, HDIM), f32)
        t_recv[...] = jnp.ones_like(t_recv)

    coef_copy.wait()
    row_copy.wait()

    lag_f = rank * LAG
    lag_b = (ranks - 1 - rank) * LAG
    lag_d = jnp.maximum(lag_f, lag_b)

    def relay_decay():
        @pl.when(jnp.logical_not(is_last))
        def _():
            t_copy.wait_recv()

        @pl.when(jnp.logical_not(is_first))
        def _():
            t_send[...] = t_recv[...] * coef_recv[...] * coef_s[side]
            t_copy.start()

    def rows_of(j, p):
        c_own = coef_s[side, p, pl.ds(j, 1), :]
        c_other = coef_recv[p, pl.ds(j, 1), :]
        return jnp.where(low, c_own, c_other), jnp.where(low, c_other, c_own)

    def combine(j, p, c):
        @pl.when((p == 0) & (c == 0))
        def _():
            for k in range(parts):
                x_copy(j, k).wait_recv()

        at = piece(c)
        base_own = jnp.where(low, base_low, base_high)
        base_other = jnp.where(low, base_high, base_low)
        own = None
        other = None
        for k in range(parts):
            a = unity(base_own + k == p) * own_part[j, k, at]
            b = unity(base_other + k == p) * x_recv[j, k, at]
            own = a if k == 0 else own + a
            other = b if k == 0 else other + b
        c_low, c_high = rows_of(j, p)
        at_low = jnp.where(low, own, other)
        low_part[j, p, at] = at_low
        pair_part[j, p, at] = c_high * at_low + jnp.where(low, other, own)

    def forward(j, p, c):
        @pl.when(jnp.logical_not(is_first) & (p < fwd))
        def _():
            f_copy(j, p, c).wait_recv()

        at = piece(c)
        c_low, c_high = rows_of(j, p)
        came = f_recv[j, p, at]
        middle = c_low * came
        f_send[j, p, at] = c_high * middle + pair_part[j, p, at]

        @pl.when(jnp.logical_not(is_last) & (p < fwd))
        def _():
            f_copy(j, p, c).start()

        at_low = came * unity(front_low == p)
        at_high = (middle + low_part[j, p, at]) * unity(front_high == p)
        to_mine = jnp.where(low, at_low, at_high)
        to_theirs = jnp.where(low, at_high, at_low)

        @pl.when(p == 0)
        def _():
            e_mine[j, at] = to_mine
            e_send[j, at] = to_theirs

        @pl.when(p > 0)
        def _():
            e_mine[j, at] += to_mine
            e_send[j, at] += to_theirs

        @pl.when((p == slots - 1) & (c == CUT - 1))
        def _():
            e_copy(j).start()

    def backward(j, p, c):
        @pl.when(jnp.logical_not(is_last) & (p >= bwd))
        def _():
            b_copy(j, p, c).wait_recv()

        @pl.when(jnp.logical_not(is_first) & (p >= bwd))
        def _():
            at = piece(c)
            t_row = t_recv[p, pl.ds(j, 1), :]
            b_send[j, p, at] = b_recv[j, p, at] + t_row * pair_part[j, p, at]
            b_copy(j, p, c).start()

    def decode(j, p):
        @pl.when(p == 0)
        def _():
            q_copy(j).wait_recv()

        t_row = t_recv[p, pl.ds(j, 1), :]
        final = (t_row * f_send[j, p] + b_recv[j, p]).astype(bf16)
        got_own = jnp.dot(sq_ref[:, lanes(mine + j)], final, preferred_element_type=f32)
        got_other = jnp.dot(q_recv[j].astype(bf16), final, preferred_element_type=f32)
        slot = p.astype(f32)
        spread = lambda a: jnp.concatenate([a] * steps, axis=0)
        got_own = jnp.where(spread(row_s[...]) == slot, got_own, 0.0)
        got_other = jnp.where(spread(row_recv[...]) == slot, got_other, 0.0)

        @pl.when(p == 0)
        def _():
            acc_own[...] = got_own
            r_send[j] = got_other

        @pl.when(p > 0)
        def _():
            acc_own[...] += got_own
            r_send[j] += got_other

        @pl.when(p == slots - 1)
        def _():
            r_copy(j).start()
            from_state(mine + j, acc_own[...])

    def split(t):
        return lax.div(t, span), lax.rem(lax.div(t, CUT), slots), lax.rem(t, CUT)

    @pl.loop(0, units + (ranks - 1) * LAG)
    def _(t):
        j, p, c = split(t)
        spot = lax.rem(t, span)

        @pl.when(t < units)
        def _():
            combine(j, p, c)

        @pl.when(t == lag_b)
        def _():
            relay_decay()

        @pl.when((t >= lag_f) & (t < units + lag_f))
        def _():
            forward(*split(t - lag_f))

        @pl.when((t >= lag_b) & (t < units + lag_b))
        def _():
            backward(*split(t - lag_b))

        @pl.when((t < units - AHEAD * span) & (spot == 0))
        def _():
            send_parts(j + AHEAD)

        @pl.when((t < units) & (spot == 1))
        def _():
            own_steps(mine + j)
            within(mine + j)

        @pl.when((t < units) & (spot == CUT))
        def _():
            own_steps(theirs + j)
            within(theirs + j)

            @pl.when(j < half - 1)
            def _():
                make_parts(mine + j + 1, j + 1, own_part)

        @pl.when((t >= lag_d) & (t < units + lag_d) & (lax.rem(t - lag_d, CUT) == CUT - 1))
        def _():
            jd, pd, _ = split(t - lag_d)
            decode(jd, pd)

        @pl.when((t >= lag_f) & (t < units + lag_f) & (lax.rem(t - lag_f, span) == span - 1))
        def _():
            jf = lax.div(t - lag_f, span)
            across(mine + jf, e_mine[jf])

    @pl.loop(0, half)
    def _(j):
        e_copy(j).wait()
        across(theirs + j, e_recv[j])

    def row_sums(acc):
        return lax.dot_general(
            jnp.ones((8, HDIM), f32),
            acc[...],
            (((1,), (1,)), ((), ())),
            precision=lax.Precision.HIGHEST,
            preferred_element_type=f32,
        )

    def scale_of(total):
        scale = lax.rsqrt(total / (n_head * width) + EPSILON)
        return jnp.transpose(scale)[:, 0:1]

    n_send[...] = row_sums(acc_sq)
    for k in range(1, n_head):
        n_copy(k).start()

    @pl.loop(0, half)
    def _(j):
        r_copy(j).wait()
        from_state(theirs + j, r_recv[j])

    d_send[...] = row_sums(acc_dsq)
    for k in range(1, n_head):
        d_copy(k).start()

    total = n_send[...]
    for k in range(1, n_head):
        n_copy(k).wait()
        total = total + n_recv[k - 1]
    scale = jnp.broadcast_to(scale_of(total), (tok, HDIM))

    @pl.loop(0, heads)
    def _(h):
        at = lanes(h)
        attn_ref[:, at] = (mixed_s[:, at] * scale * gain_ref[:, at]).astype(bf16)

    total = d_send[...]
    for k in range(1, n_head):
        d_copy(k).wait()
        total = total + d_recv[k - 1]
    dec_scale = scale_of(total)
    out_ref[...] = (dec_s[...] * dec_scale * gain_ref[...]).astype(bf16)

    @pl.loop(0, half)
    def _(j):
        q_copy(j).wait_send()
        for k in range(parts):
            x_copy(j, k).wait_send()

        for c in range(CUT):
            for p in range(fwd):

                @pl.when(jnp.logical_not(is_last))
                def _():
                    f_copy(j, p, c).wait_send()

            for p in range(bwd, slots):

                @pl.when(jnp.logical_not(is_first))
                def _():
                    b_copy(j, p, c).wait_send()

    @pl.when(jnp.logical_not(is_first))
    def _():
        t_copy.wait_send()


def fused(n, n_head, steps, variant, collective, *operands):
    parts, fwd, bwd = variant
    query, decay, step, step_decay = operands[2], operands[5], operands[7], operands[10]
    tok, width = query.shape
    heads = decay.shape[0]
    half = heads // PAIR
    vectors = step.shape[0]
    rows = vectors // steps
    slots = PROMPTS
    f32, bf16 = jnp.float32, jnp.bfloat16
    vmem = pl.BlockSpec(memory_space=pltpu.VMEM)
    smem = pl.BlockSpec(memory_space=pltpu.SMEM)
    dma = pltpu.SemaphoreType.DMA
    buffer = lambda *shape: pltpu.VMEM(shape, f32)
    states = buffer(half, slots, HDIM, HDIM)
    pieces = buffer(half, parts, HDIM, HDIM)
    decays = buffer(slots, half, HDIM)
    entries = buffer(half, HDIM, HDIM)
    products = buffer(half, vectors, HDIM)
    return pl.pallas_call(
        functools.partial(fused_kernel, n, n_head, steps, parts, fwd, bwd),
        out_shape=(
            jax.ShapeDtypeStruct((tok, width), bf16),
            jax.ShapeDtypeStruct((vectors, width), bf16),
        ),
        in_specs=[smem] * 2 + [vmem] * (len(operands) - 2),
        out_specs=(vmem,) * 2,
        scratch_shapes=[
            buffer(heads, 8, tok),
            buffer(tok, tok),
            buffer(steps * (steps + 1) // 2, rows, heads),
            buffer(PAIR, slots, half, HDIM),
            decays,
            buffer(rows, HDIM),
            buffer(rows, HDIM),
            buffer(tok, width),
            buffer(vectors, width),
            pieces,
            pieces,
            pieces,
            products,
            products,
            states,
            states,
            states,
            states,
            states,
            states,
            decays,
            decays,
            entries,
            buffer(tok, HDIM),
            buffer(vectors, HDIM),
            buffer(vectors, HDIM),
            entries,
            entries,
            products,
            products,
            buffer(8, tok),
            buffer(n_head - 1, 8, tok),
            buffer(8, vectors),
            buffer(n_head - 1, 8, vectors),
            dma((half * parts,)),
            dma((half * parts,)),
            dma,
            dma,
            dma((half,)),
            dma((half,)),
            dma,
            dma,
            dma((half * slots * CUT,)),
            dma((half * slots * CUT,)),
            dma((half * slots * CUT,)),
            dma((half * slots * CUT,)),
            dma,
            dma,
            dma((half,)),
            dma((half,)),
            dma((half,)),
            dma((half,)),
            dma((n_head - 1,)),
            dma((n_head - 1,)),
            dma((n_head - 1,)),
            dma((n_head - 1,)),
        ],
        compiler_params=pltpu.CompilerParams(
            collective_id=collective, has_side_effects=True, vmem_limit_bytes=56 * 1024 * 1024
        ),
        name="fused",
    )(*operands)


def pick_kernel(n, tok, lens_ref, index_ref):
    number = lambda flag: jnp.where(flag, 1, 0).astype(jnp.int32)
    ends = []
    for p in range(PROMPTS):
        ends.append(lens_ref[p] + (ends[-1] if p else 0))

    def crowd(d, most):
        met = 0
        for p in range(PROMPTS):
            met = met + number((ends[p] - lens_ref[p] < (d + 1) * tok) & (ends[p] > d * tok))
        return jnp.maximum(most, met)

    most = jnp.int32(0)
    for d in range(n):
        most = crowd(d, most)
    early = ends[0] < PAIR * tok
    late = ends[PROMPTS - 2] >= (n - PAIR) * tok
    narrow = number(early & late) * 2 + number(most > 2)
    index_ref[0] = jnp.where(most > 3, len(VARIANTS) - 1, narrow)


def variant_of(n, tok, prompt_lengths):
    smem = pl.BlockSpec(memory_space=pltpu.SMEM)
    index = pl.pallas_call(
        functools.partial(pick_kernel, n, tok),
        out_shape=jax.ShapeDtypeStruct((1,), jnp.int32),
        in_specs=[smem],
        out_specs=smem,
        name="pick",
    )(prompt_lengths)
    return index[0]


def local(
    n,
    n_head,
    query_in,
    key_in,
    value_in,
    log_decay,
    norm_gain,
    prompt_lengths,
    step_query,
    step_key,
    step_value,
    step_decay,
    row_prompt,
):
    steps, rows = step_query.shape[:2]
    flat = lambda a: a.reshape(steps * rows, -1)
    operands = (
        prompt_lengths,
        row_prompt,
        query_in,
        key_in,
        value_in,
        log_decay.T,
        norm_gain[None, :],
        flat(step_query),
        flat(step_key),
        flat(step_value),
        step_decay,
    )
    branches = [
        functools.partial(fused, n, n_head, steps, variant, i) for i, variant in enumerate(VARIANTS)
    ]
    attn_out, decode_out = lax.switch(
        variant_of(n, query_in.shape[0], prompt_lengths), branches, *operands
    )
    return (attn_out, decode_out.reshape(step_query.shape))


def solution(mesh):
    in_specs = (
        P("seq", "head"),
        P("seq", "head"),
        P("seq", "head"),
        P("seq", "head"),
        P("head"),
        P(),
        P(None, "seq", "head"),
        P(None, "seq", "head"),
        P(None, "seq", "head"),
        P(None, "seq", "head"),
        P("seq"),
    )
    out_specs = (P("seq", "head"), P(None, "seq", "head"))
    return jax.shard_map(
        functools.partial(local, mesh.shape["seq"], mesh.shape["head"]),
        mesh=mesh,
        in_specs=in_specs,
        out_specs=out_specs,
        check_vma=False,
    )
```

```python
import functools

import jax
import jax.numpy as jnp
from jax import lax
from jax.experimental import pallas as pl
from jax.experimental.pallas import tpu as pltpu
from jax.sharding import PartitionSpec as P

HDIM = 128
PROMPTS = 4
PAIR = 2
CUT = 1
AHEAD = 3
BACK = 4
WIDE = (4, 0, 3)
NARROW = (3, 1, 4)
VARIANTS = ((2,) + WIDE, (3,) + WIDE, (2,) + NARROW, (3,) + NARROW, (4,) + WIDE)
CUM_ROW = 4
CARRIED_ROW = 5

EPSILON = 1e-06
MESH = pl.DeviceIdType.MESH


def fused_kernel(
    n,
    n_head,
    steps,
    parts,
    fwd,
    bwd,
    lag,
    lens_ref,
    prompt_ref,
    query_ref,
    key_ref,
    value_ref,
    decay_ref,
    gain_ref,
    sq_ref,
    sk_ref,
    sv_ref,
    sd_ref,
    attn_ref,
    out_ref,
    gain_s,
    gain_sem,
    token_s,
    bias_s,
    weight_s,
    coef_s,
    coef_recv,
    row_s,
    row_recv,
    mixed_s,
    dec_s,
    own_part,
    x_send,
    x_recv,
    q_send,
    q_recv,
    f_recv,
    f_send,
    b_recv,
    b_send,
    pair_part,
    low_part,
    t_recv,
    t_send,
    e_mine,
    acc_sq,
    acc_dsq,
    acc_own,
    e_send,
    e_recv,
    r_send,
    r_recv,
    n_send,
    n_recv,
    d_send,
    d_recv,
    xs_sem,
    xr_sem,
    cs_sem,
    cr_sem,
    qs_sem,
    qr_sem,
    ws_sem,
    wr_sem,
    fs_sem,
    fr_sem,
    bs_sem,
    br_sem,
    ts_sem,
    tr_sem,
    es_sem,
    er_sem,
    rs_sem,
    rr_sem,
    ns_sem,
    nr_sem,
    ds_sem,
    dr_sem,
):
    f32, bf16, i32 = jnp.float32, jnp.bfloat16, jnp.int32
    me = lax.axis_index("seq")
    hd = lax.axis_index("head")
    side = lax.rem(me, PAIR)
    rank = lax.div(me, PAIR)
    ranks = n // PAIR
    partner = me + 1 - 2 * side
    half = own_part.shape[0]
    heads = PAIR * half
    tok, width = query_ref.shape
    slots = PROMPTS
    span = slots * CUT
    units = half * span
    back = min(BACK, half)
    cut = HDIM // CUT
    rows = sq_ref.shape[0] // steps
    mine = side * half
    theirs = (1 - side) * half
    is_first = rank == 0
    is_last = rank == ranks - 1
    low = side == 0
    ahead = lax.rem(me + PAIR, n)
    behind = lax.rem(me + n - PAIR, n)

    def copy(src, dst, send, recv, to):
        return pltpu.make_async_remote_copy(
            src_ref=src,
            dst_ref=dst,
            send_sem=send,
            recv_sem=recv,
            device_id=to,
            device_id_type=MESH,
        )

    def x_copy(j, k):
        i = j * parts + k
        return copy(
            x_send.at[j, k], x_recv.at[j, k], xs_sem.at[i], xr_sem.at[i], {"seq": partner}
        )

    def piece(c):
        return pl.ds(pl.multiple_of(c * cut, cut), cut)

    def f_copy(j, p, c):
        i, at = j * span + p * CUT + c, piece(c)
        return copy(
            f_send.at[j, p, at], f_recv.at[j, p, at], fs_sem.at[i], fr_sem.at[i], {"seq": ahead}
        )

    def b_copy(j, p, c):
        i, at = j * span + p * CUT + c, piece(c)
        return copy(
            b_send.at[j, p, at], b_recv.at[j, p, at], bs_sem.at[i], br_sem.at[i], {"seq": behind}
        )

    def q_copy(j):
        return copy(q_send.at[j], q_recv.at[j], qs_sem.at[j], qr_sem.at[j], {"seq": partner})

    def e_copy(j):
        return copy(e_send.at[j], e_recv.at[j], es_sem.at[j], er_sem.at[j], {"seq": partner})

    def r_copy(j):
        return copy(r_send.at[j], r_recv.at[j], rs_sem.at[j], rr_sem.at[j], {"seq": partner})

    def peer(k):
        return {"head": lax.rem(hd + k, n_head)}

    def n_copy(k):
        return copy(n_send, n_recv.at[k - 1], ns_sem.at[k - 1], nr_sem.at[k - 1], peer(k))

    def d_copy(k):
        return copy(d_send, d_recv.at[k - 1], ds_sem.at[k - 1], dr_sem.at[k - 1], peer(k))

    coef_copy = copy(coef_s.at[1 - side], coef_recv, cs_sem, cr_sem, {"seq": partner})
    row_copy = copy(row_s, row_recv, ws_sem, wr_sem, {"seq": partner})
    t_copy = copy(t_send, t_recv, ts_sem, tr_sem, {"seq": behind})

    def lanes(h):
        return pl.ds(pl.multiple_of(h * HDIM, HDIM), HDIM)

    gain_copy = pltpu.make_async_copy(gain_ref, gain_s, gain_sem)
    gain_copy.start()
    barrier = pltpu.get_barrier_semaphore()

    def greet(to):
        pl.semaphore_signal(barrier, inc=1, device_id=to, device_id_type=MESH)

    greet({"seq": partner})
    for k in range(1, n_head):
        greet(peer(k))

    @pl.when(jnp.logical_not(is_last))
    def _():
        greet({"seq": ahead})

    @pl.when(jnp.logical_not(is_first))
    def _():
        greet({"seq": behind})

    ends = []
    for p in range(slots):
        ends.append(lens_ref[p] + (ends[-1] if p else 0))
    begins = [ends[p] - lens_ref[p] for p in range(slots)]

    def number(flag):
        return jnp.where(flag, 1, 0).astype(i32)

    def unity(flag):
        return jnp.where(flag, 1.0, 0.0).astype(f32)

    def seg_of(token):
        total = number(token >= ends[0])
        for p in range(1, slots):
            total = total + number(token >= ends[p])
        return total

    def seg_before(token):
        return jnp.where(token > 0, seg_of(token - 1), -1)

    first = me * tok
    pair_first = rank * (PAIR * tok)
    base = seg_of(first)
    base_low = seg_of(pair_first)
    base_high = seg_of(pair_first + tok)
    front_low = seg_before(pair_first)
    front_high = seg_before(pair_first + tok)

    sub = lax.broadcasted_iota(i32, (tok, tok), 0)
    lane = lax.broadcasted_iota(i32, (tok, tok), 1)
    cum = jnp.dot(
        decay_ref[...],
        jnp.where(sub <= lane, 1.0, 0.0).astype(f32),
        precision=lax.Precision.HIGHEST,
        preferred_element_type=f32,
    )
    place = lax.broadcasted_iota(i32, (heads, tok), 1)
    segs = seg_of(place + first)
    goal = jnp.zeros_like(cum)
    for p in range(slots):
        last = jnp.clip(ends[p] - first, 1, tok) - 1
        reached = jnp.sum(jnp.where(place == last, cum, 0.0), axis=1, keepdims=True)
        goal = jnp.where(segs == p, reached, goal)
        grown = jnp.where(begins[p] < first, jnp.exp(reached), 0.0)
        coef = jnp.where(ends[p] <= first, 1.0, grown)
        coef = jnp.broadcast_to(coef, (heads, HDIM))
        for s in range(PAIR):
            coef_s[s, p] = coef[s * half : (s + 1) * half]
    keep = jnp.exp(goal - cum)
    carried = jnp.where(segs == seg_before(first), jnp.exp(cum), 0.0)
    keeps = [jnp.where(segs == base + k, keep, 0.0) for k in range(parts)]
    token_s[...] = jnp.zeros_like(token_s)
    for h in range(heads):
        at = slice(h, h + 1)
        for k in range(parts):
            token_s[h, k : k + 1, :] = keeps[k][at]
        token_s[h, CUM_ROW : CUM_ROW + 1, :] = cum[at]
        token_s[h, CARRIED_ROW : CARRIED_ROW + 1, :] = carried[at]

    def make_parts(h, j, into):
        key = key_ref[:, lanes(h)].astype(f32)
        value = value_ref[:, lanes(h)]
        cols = jnp.transpose(token_s[h])
        for k in range(parts):
            keyed = (key * cols[:, k : k + 1]).astype(bf16)
            into[j, k] = lax.dot_general(
                keyed, value, (((0,), (0,)), ((), ())), preferred_element_type=f32
            )

    def within(h):
        query = query_ref[:, lanes(h)]
        scores = lax.dot_general(
            query, key_ref[:, lanes(h)], (((1,), (1,)), ((), ())), preferred_element_type=f32
        )
        cols = jnp.transpose(token_s[h])
        column = cols[:, CUM_ROW : CUM_ROW + 1]
        spread = column - token_s[h, CUM_ROW : CUM_ROW + 1, :] + bias_s[...]
        weights = (scores * jnp.exp(spread)).astype(bf16)
        mixed_s[:, lanes(h)] = jnp.dot(
            weights, value_ref[:, lanes(h)], preferred_element_type=f32
        )

    def across(h, entry):
        column = jnp.transpose(token_s[h])[:, CARRIED_ROW : CARRIED_ROW + 1]
        outer = jnp.dot(query_ref[:, lanes(h)], entry.astype(bf16), preferred_element_type=f32)
        mixed = mixed_s[:, lanes(h)] + outer * column
        mixed_s[:, lanes(h)] = mixed
        acc_sq[...] += mixed * mixed

    pick = lax.broadcasted_iota(i32, (rows, heads), 1)

    def weight_col(i, h):
        return jnp.sum(jnp.where(pick == h, weight_s[i], 0.0), axis=1, keepdims=True)

    def own_steps(h):
        query = sq_ref[:, lanes(h)].astype(f32)
        key = sk_ref[:, lanes(h)].astype(f32)
        value = sv_ref[:, lanes(h)].astype(f32)
        step = lambda a, i: a[i * rows : (i + 1) * rows]
        spot = steps
        for i in range(steps):
            total = None
            for j in range(i + 1):
                dot = jnp.sum(step(query, i) * step(key, j), axis=1, keepdims=True)
                if j < i:
                    dot = dot * weight_col(spot, h)
                    spot += 1
                term = dot * step(value, j)
                total = term if j == 0 else total + term
            dec_s[i * rows : (i + 1) * rows, lanes(h)] = total

    def from_state(h, product):
        for i in range(steps):
            at = slice(i * rows, (i + 1) * rows)
            out = dec_s[at, lanes(h)] + weight_col(i, h) * product[at]
            dec_s[at, lanes(h)] = out
            acc_dsq[at] += out * out

    def send_parts(j):
        make_parts(theirs + j, j, x_send)
        for k in range(parts):
            x_copy(j, k).start()

    def send_query(j):
        q_send[j] = sq_ref[:, lanes(theirs + j)].astype(f32)
        q_copy(j).start()

    make_parts(theirs, 0, x_send)
    pl.semaphore_wait(
        barrier, n_head + jnp.where(is_first, 0, 1) + jnp.where(is_last, 0, 1)
    )
    coef_copy.start()
    for k in range(parts):
        x_copy(0, k).start()
    make_parts(mine, 0, own_part)

    column = lax.broadcasted_iota(i32, (rows, HDIM), 0)
    marks = jnp.zeros((rows, HDIM), f32)
    for r in range(rows):
        marks = jnp.where(column == r, prompt_ref[r].astype(f32), marks)
    row_s[...] = marks
    row_copy.start()
    tops = jnp.broadcast_to(segs[0:1].astype(f32), (8, tok))
    linked = (sub >= lane) & (jnp.transpose(tops)[:, 0:1] == tops[0:1])
    bias_s[...] = jnp.where(linked, 0.0, -jnp.inf)
    totals = []
    for i in range(steps):
        totals.append(sd_ref[i] + totals[-1] if i else sd_ref[i])
    spot = steps
    for i in range(steps):
        weight_s[i] = jnp.exp(totals[i])
        for j in range(i):
            weight_s[spot] = jnp.exp(totals[i] - totals[j])
            spot += 1
    acc_sq[...] = jnp.zeros_like(acc_sq)
    acc_dsq[...] = jnp.zeros_like(acc_dsq)
    if fwd < slots:
        f_recv[:, fwd:] = jnp.zeros((half, slots - fwd, HDIM, HDIM), f32)
    if bwd > 0:
        b_recv[:, :bwd] = jnp.zeros((half, bwd, HDIM, HDIM), f32)

    @pl.when(is_first)
    def _():
        f_recv[:, :fwd] = jnp.zeros((half, fwd, HDIM, HDIM), f32)

    @pl.when(is_last)
    def _():
        b_recv[:, bwd:] = jnp.zeros((half, slots - bwd, HDIM, HDIM), f32)
        t_recv[...] = jnp.ones_like(t_recv)

    coef_copy.wait()
    row_copy.wait()

    lag_f = rank * lag
    lag_b = (ranks - 1 - rank) * lag
    lag_d = jnp.maximum(lag_f, lag_b)

    def relay_decay():
        @pl.when(jnp.logical_not(is_last))
        def _():
            t_copy.wait_recv()

        @pl.when(jnp.logical_not(is_first))
        def _():
            t_send[...] = t_recv[...] * coef_recv[...] * coef_s[side]
            t_copy.start()

    def rows_of(j, p):
        c_own = coef_s[side, p, pl.ds(j, 1), :]
        c_other = coef_recv[p, pl.ds(j, 1), :]
        return jnp.where(low, c_own, c_other), jnp.where(low, c_other, c_own)

    def combine(j, p, c):
        @pl.when((p == 0) & (c == 0))
        def _():
            for k in range(parts):
                x_copy(j, k).wait_recv()

        at = piece(c)
        base_own = jnp.where(low, base_low, base_high)
        base_other = jnp.where(low, base_high, base_low)
        own = None
        other = None
        for k in range(parts):
            a = unity(base_own + k == p) * own_part[j, k, at]
            b = unity(base_other + k == p) * x_recv[j, k, at]
            own = a if k == 0 else own + a
            other = b if k == 0 else other + b
        c_low, c_high = rows_of(j, p)
        at_low = jnp.where(low, own, other)
        low_part[j, p, at] = at_low
        pair_part[j, p, at] = c_high * at_low + jnp.where(low, other, own)

    def forward(j, p, c):
        @pl.when(jnp.logical_not(is_first) & (p < fwd))
        def _():
            f_copy(j, p, c).wait_recv()

        at = piece(c)
        c_low, c_high = rows_of(j, p)
        came = f_recv[j, p, at]
        middle = c_low * came
        f_send[j, p, at] = c_high * middle + pair_part[j, p, at]

        @pl.when(jnp.logical_not(is_last) & (p < fwd))
        def _():
            f_copy(j, p, c).start()

        at_low = came * unity(front_low == p)
        at_high = (middle + low_part[j, p, at]) * unity(front_high == p)
        to_mine = jnp.where(low, at_low, at_high)
        to_theirs = jnp.where(low, at_high, at_low)

        @pl.when(p == 0)
        def _():
            e_mine[j, at] = to_mine
            e_send[j, at] = to_theirs

        @pl.when(p > 0)
        def _():
            e_mine[j, at] += to_mine
            e_send[j, at] += to_theirs

        @pl.when((p == slots - 1) & (c == CUT - 1))
        def _():
            e_copy(j).start()

    def backward(j, p, c):
        @pl.when(jnp.logical_not(is_last) & (p >= bwd))
        def _():
            b_copy(j, p, c).wait_recv()

        @pl.when(jnp.logical_not(is_first) & (p >= bwd))
        def _():
            at = piece(c)
            t_row = t_recv[p, pl.ds(j, 1), :]
            b_send[j, p, at] = b_recv[j, p, at] + t_row * pair_part[j, p, at]
            b_copy(j, p, c).start()

    def decode(j, p):
        @pl.when(p == 0)
        def _():
            q_copy(j).wait_recv()

        t_row = t_recv[p, pl.ds(j, 1), :]
        final = (t_row * f_send[j, p] + b_recv[j, p]).astype(bf16)
        got_own = jnp.dot(sq_ref[:, lanes(mine + j)], final, preferred_element_type=f32)
        got_other = jnp.dot(q_recv[j].astype(bf16), final, preferred_element_type=f32)
        slot = p.astype(f32)
        spread = lambda a: jnp.concatenate([a] * steps, axis=0)
        got_own = jnp.where(spread(row_s[...]) == slot, got_own, 0.0)
        got_other = jnp.where(spread(row_recv[...]) == slot, got_other, 0.0)

        @pl.when(p == 0)
        def _():
            acc_own[...] = got_own
            r_send[j] = got_other

        @pl.when(p > 0)
        def _():
            acc_own[...] += got_own
            r_send[j] += got_other

        @pl.when(p == slots - 1)
        def _():
            r_copy(j).start()
            from_state(mine + j, acc_own[...])

            @pl.when(j >= back)
            def _():
                from_partner(j - back)

    def across_theirs(j):
        e_copy(j).wait()
        across(theirs + j, e_recv[j])

    def from_partner(j):
        r_copy(j).wait()
        from_state(theirs + j, r_recv[j])

    def split(t):
        return lax.div(t, span), lax.rem(lax.div(t, CUT), slots), lax.rem(t, CUT)

    @pl.loop(0, units + (ranks - 1) * lag)
    def _(t):
        j, p, c = split(t)
        spot = lax.rem(t, span)

        @pl.when(t < units)
        def _():
            combine(j, p, c)

        @pl.when(t == lag_b)
        def _():
            relay_decay()

        @pl.when((t >= lag_f) & (t < units + lag_f))
        def _():
            forward(*split(t - lag_f))

        @pl.when((t >= lag_b) & (t < units + lag_b))
        def _():
            backward(*split(t - lag_b))

        @pl.when((t > 0) & (t < AHEAD))
        def _():
            send_parts(t)

        @pl.when((t < units - AHEAD * span) & (spot == AHEAD))
        def _():
            send_parts(j + AHEAD)

        @pl.when((t < units) & (spot == CUT))
        def _():
            send_query(j)

        @pl.when((t < units) & (spot == 1))
        def _():
            own_steps(mine + j)
            within(mine + j)

        @pl.when((t < units) & (spot == CUT))
        def _():
            own_steps(theirs + j)
            within(theirs + j)

            @pl.when(j < half - 1)
            def _():
                make_parts(mine + j + 1, j + 1, own_part)

        @pl.when((t >= lag_d) & (t < units + lag_d) & (lax.rem(t - lag_d, CUT) == CUT - 1))
        def _():
            jd, pd, _ = split(t - lag_d)
            decode(jd, pd)

        @pl.when((t >= lag_f) & (t < units + lag_f) & (lax.rem(t - lag_f, span) == span - 1))
        def _():
            jf = lax.div(t - lag_f, span)
            across(mine + jf, e_mine[jf])

            @pl.when(jf >= back)
            def _():
                across_theirs(jf - back)

    pl.loop(half - back, half)(across_theirs)

    def row_sums(acc):
        return lax.dot_general(
            jnp.ones((8, HDIM), f32),
            acc[...],
            (((1,), (1,)), ((), ())),
            precision=lax.Precision.HIGHEST,
            preferred_element_type=f32,
        )

    def scale_of(total):
        scale = lax.rsqrt(total / (n_head * width) + EPSILON)
        return jnp.transpose(scale)[:, 0:1]

    n_send[...] = row_sums(acc_sq)
    for k in range(1, n_head):
        n_copy(k).start()

    pl.loop(half - back, half)(from_partner)

    d_send[...] = row_sums(acc_dsq)
    for k in range(1, n_head):
        d_copy(k).start()

    total = n_send[...]
    for k in range(1, n_head):
        n_copy(k).wait()
        total = total + n_recv[k - 1]
    scale = jnp.broadcast_to(scale_of(total), (tok, HDIM))
    gain_copy.wait()

    @pl.loop(0, heads)
    def _(h):
        at = lanes(h)
        attn_ref[:, at] = (mixed_s[:, at] * scale * gain_s[:, at]).astype(bf16)

    total = d_send[...]
    for k in range(1, n_head):
        d_copy(k).wait()
        total = total + d_recv[k - 1]
    dec_scale = scale_of(total)
    out_ref[...] = (dec_s[...] * dec_scale * gain_s[...]).astype(bf16)

    @pl.loop(0, half)
    def _(j):
        q_copy(j).wait_send()
        for k in range(parts):
            x_copy(j, k).wait_send()

        for c in range(CUT):
            for p in range(fwd):

                @pl.when(jnp.logical_not(is_last))
                def _():
                    f_copy(j, p, c).wait_send()

            for p in range(bwd, slots):

                @pl.when(jnp.logical_not(is_first))
                def _():
                    b_copy(j, p, c).wait_send()

    @pl.when(jnp.logical_not(is_first))
    def _():
        t_copy.wait_send()


def fused(n, n_head, steps, variant, collective, *operands):
    parts, fwd, bwd, lag = variant
    query, decay, step, step_decay = operands[2], operands[5], operands[7], operands[10]
    tok, width = query.shape
    heads = decay.shape[0]
    half = heads // PAIR
    vectors = step.shape[0]
    rows = vectors // steps
    slots = PROMPTS
    f32, bf16 = jnp.float32, jnp.bfloat16
    vmem = pl.BlockSpec(memory_space=pltpu.VMEM)
    smem = pl.BlockSpec(memory_space=pltpu.SMEM)
    hbm = pl.BlockSpec(memory_space=pltpu.HBM)
    dma = pltpu.SemaphoreType.DMA
    buffer = lambda *shape: pltpu.VMEM(shape, f32)
    states = buffer(half, slots, HDIM, HDIM)
    pieces = buffer(half, parts, HDIM, HDIM)
    decays = buffer(slots, half, HDIM)
    entries = buffer(half, HDIM, HDIM)
    products = buffer(half, vectors, HDIM)
    return pl.pallas_call(
        functools.partial(fused_kernel, n, n_head, steps, parts, fwd, bwd, lag),
        out_shape=(
            jax.ShapeDtypeStruct((tok, width), bf16),
            jax.ShapeDtypeStruct((vectors, width), bf16),
        ),
        in_specs=[hbm if i == 6 else smem if i < 2 else vmem for i in range(len(operands))],
        out_specs=(vmem,) * 2,
        scratch_shapes=[
            buffer(1, width),
            dma,
            buffer(heads, 8, tok),
            buffer(tok, tok),
            buffer(steps * (steps + 1) // 2, rows, heads),
            buffer(PAIR, slots, half, HDIM),
            decays,
            buffer(rows, HDIM),
            buffer(rows, HDIM),
            buffer(tok, width),
            buffer(vectors, width),
            pieces,
            pieces,
            pieces,
            products,
            products,
            states,
            states,
            states,
            states,
            states,
            states,
            decays,
            decays,
            entries,
            buffer(tok, HDIM),
            buffer(vectors, HDIM),
            buffer(vectors, HDIM),
            entries,
            entries,
            products,
            products,
            buffer(8, tok),
            buffer(n_head - 1, 8, tok),
            buffer(8, vectors),
            buffer(n_head - 1, 8, vectors),
            dma((half * parts,)),
            dma((half * parts,)),
            dma,
            dma,
            dma((half,)),
            dma((half,)),
            dma,
            dma,
            dma((half * slots * CUT,)),
            dma((half * slots * CUT,)),
            dma((half * slots * CUT,)),
            dma((half * slots * CUT,)),
            dma,
            dma,
            dma((half,)),
            dma((half,)),
            dma((half,)),
            dma((half,)),
            dma((n_head - 1,)),
            dma((n_head - 1,)),
            dma((n_head - 1,)),
            dma((n_head - 1,)),
        ],
        compiler_params=pltpu.CompilerParams(
            collective_id=collective, has_side_effects=True, vmem_limit_bytes=56 * 1024 * 1024
        ),
        name="fused",
    )(*operands)


def pick_kernel(n, tok, lens_ref, index_ref):
    number = lambda flag: jnp.where(flag, 1, 0).astype(jnp.int32)
    ends = []
    for p in range(PROMPTS):
        ends.append(lens_ref[p] + (ends[-1] if p else 0))

    def crowd(d, most):
        met = 0
        for p in range(PROMPTS):
            met = met + number((ends[p] - lens_ref[p] < (d + 1) * tok) & (ends[p] > d * tok))
        return jnp.maximum(most, met)

    most = jnp.int32(0)
    for d in range(n):
        most = crowd(d, most)
    early = ends[0] < PAIR * tok
    late = ends[PROMPTS - 2] >= (n - PAIR) * tok
    narrow = number(early & late) * 2 + number(most > 2)
    index_ref[0] = jnp.where(most > 3, len(VARIANTS) - 1, narrow)


def variant_of(n, tok, prompt_lengths):
    smem = pl.BlockSpec(memory_space=pltpu.SMEM)
    index = pl.pallas_call(
        functools.partial(pick_kernel, n, tok),
        out_shape=jax.ShapeDtypeStruct((1,), jnp.int32),
        in_specs=[smem],
        out_specs=smem,
        name="pick",
    )(prompt_lengths)
    return index[0]


def local(
    n,
    n_head,
    query_in,
    key_in,
    value_in,
    log_decay,
    norm_gain,
    prompt_lengths,
    step_query,
    step_key,
    step_value,
    step_decay,
    row_prompt,
):
    steps, rows = step_query.shape[:2]
    flat = lambda a: a.reshape(steps * rows, -1)
    operands = (
        prompt_lengths,
        row_prompt,
        query_in,
        key_in,
        value_in,
        log_decay.T,
        norm_gain[None, :],
        flat(step_query),
        flat(step_key),
        flat(step_value),
        step_decay,
    )
    branches = [
        functools.partial(fused, n, n_head, steps, variant, i) for i, variant in enumerate(VARIANTS)
    ]
    attn_out, decode_out = lax.switch(
        variant_of(n, query_in.shape[0], prompt_lengths), branches, *operands
    )
    return (attn_out, decode_out.reshape(step_query.shape))


def solution(mesh):
    in_specs = (
        P("seq", "head"),
        P("seq", "head"),
        P("seq", "head"),
        P("seq", "head"),
        P("head"),
        P(),
        P(None, "seq", "head"),
        P(None, "seq", "head"),
        P(None, "seq", "head"),
        P(None, "seq", "head"),
        P("seq"),
    )
    out_specs = (P("seq", "head"), P(None, "seq", "head"))
    return jax.shard_map(
        functools.partial(local, mesh.shape["seq"], mesh.shape["head"]),
        mesh=mesh,
        in_specs=in_specs,
        out_specs=out_specs,
        check_vma=False,
    )
```
